32 devices in a mesh: grp: 4 (over x, core), sub: 8 (over z, y).
Axes of the slice: x: 2, y: 2, z: 4, core: 2. Of those that a mesh axis runs over, the one named last changes fastest.
Arguments:
- snapshots: bfloat16 [2048, 2, 32, 128], P(None, None, ('grp', 'sub')), may hold values from -6 to 6
- steering: bfloat16 [32, 2, 128, 64], P(('grp', 'sub')), may hold values from -0.375 to 0.375
- combining: bfloat16 [32, 2, 64, 1024], P(('grp', 'sub')), may hold values from -0.09375 to 0.09375
- beam_list: int32 [1024], replicated, may hold values from 0 to 1023, each once
Outputs:
- beams_out: bfloat16 [2, 2048, 1024], P(None, ('grp', 'sub'))
The draws below stay inside these ranges and needn't reach their ends.
Inputs may be any that keep to these rules, and one draw needn't show every extreme that they name: `beam_list`: each of the 1024 beams appears once.
All inputs are finite; a program needn't handle non-finite values.
Results may differ from the reference program's by a relative error of at most 0.0065.
Values may be sent and summed in bfloat16 or wider, within the bound.
A program may use at most 128 MiB of HBM per device.

```python
import jax
import jax.numpy as jnp
from jax import lax

EL = 128
PB = 64
NBEAM = 1024
SNAP = 2048
SUBS = 32


def level_of(stream_key, extent, pieces, smallest, largest):
    def one(dim, blocks):
        draws = jax.random.uniform(jax.random.fold_in(jax.random.fold_in(stream_key, 6), dim), (blocks,), jnp.float32, smallest / len(pieces), largest / len(pieces))
        return jnp.repeat(jnp.exp(draws), extent[dim] // blocks).reshape((-1,) + (1,) * (len(extent) - dim - 1))

    factor_of = one(*pieces[0])
    for cut in pieces[1:]:
        factor_of = factor_of * one(*cut)
    return factor_of


def noise(rng, dims, width, limit, shards=(), kind=jnp.bfloat16):
    result = jax.random.normal(rng, dims, jnp.float32) * width
    if len(shards) > 0:
        result = level_of(rng, dims, shards, -0.22, 0.18) * result
    return jnp.clip(result, min=-limit, max=limit).astype(kind)


def setup_inputs(seed: int = 0) -> dict:
    keys = jax.random.split(jax.random.key(seed), 5)
    return {
        "snapshots": noise(keys[0], (SNAP, 2, SUBS, EL), 1.0, 6.0, ((2, 32),)),
        "steering": noise(keys[1], (SUBS, 2, EL, PB), (2 * EL) ** -0.5, 0.375, ((0, 32),)),
        "combining": noise(keys[2], (SUBS, 2, PB, NBEAM), (2 * SUBS * PB) ** -0.5, 0.09375, ((0, 32),)),
        "beam_list": jax.random.permutation(keys[3], NBEAM).astype(jnp.int32),
    }


def reference(snapshots, steering, combining, beam_list):
    ordered = jnp.take(combining, beam_list, axis=3)

    def accumulate(subarray, running):
        signal = lax.dynamic_index_in_dim(snapshots, subarray, 2, keepdims=False).astype(jnp.float32)
        steer_s = lax.dynamic_index_in_dim(steering, subarray, 0, keepdims=False).astype(jnp.float32)
        comb_s = lax.dynamic_index_in_dim(ordered, subarray, 0, keepdims=False).astype(jnp.float32)
        sig_real = signal[:, 0]
        sig_imag = signal[:, 1]
        beam_real = jnp.dot(sig_real, steer_s[0]) - jnp.dot(sig_imag, steer_s[1])
        beam_imag = jnp.dot(sig_real, steer_s[1]) + jnp.dot(sig_imag, steer_s[0])
        beam_real = lax.optimization_barrier(beam_real.astype(jnp.bfloat16)).astype(jnp.float32)
        beam_imag = lax.optimization_barrier(beam_imag.astype(jnp.bfloat16)).astype(jnp.float32)
        final_real = jnp.dot(beam_real, comb_s[0]) - jnp.dot(beam_imag, comb_s[1])
        final_imag = jnp.dot(beam_real, comb_s[1]) + jnp.dot(beam_imag, comb_s[0])
        return running + jnp.stack([final_real, final_imag])

    running = lax.fori_loop(0, SUBS, accumulate, jnp.zeros((2, SNAP, NBEAM), jnp.float32))
    return running.astype(jnp.bfloat16)
```

```python
import functools

import jax
import jax.numpy as jnp
from jax import lax
from jax.experimental import pallas as pl
from jax.experimental.pallas import tpu as pltpu
from jax.sharding import PartitionSpec as P

MESH = pl.DeviceIdType.MESH
F32 = jnp.float32
BF16 = jnp.bfloat16
LAG = 3
AHEAD = 3
SECOND = 3
VMEM_LIMIT = 63 * 1024 * 1024


class Plan:
    def __init__(self, mesh, snap, width, beams):
        self.grp = mesh.shape["grp"]
        self.sub = mesh.shape["sub"]
        self.cores = 2 if self.grp % 2 == 0 else 1
        self.nx = self.grp // self.cores
        self.halves, self.pair = 2, 2
        self.hi = self.halves * self.pair
        self.lo = self.sub // self.hi
        self.block = snap // (self.grp * self.sub)
        self.width = width
        self.beams = beams
        self.chunks = 8 if beams % 1024 == 0 else 1
        self.cols = beams // self.chunks
        self.offsets = [(dx, dy) for dx in range(self.nx) for dy in range(self.lo)]
        self.slots = len(self.offsets) * self.cores
        self.rows_h = self.pair * self.lo * self.block


def beam_kernel(
    plan,
    x_hbm,
    s_hbm,
    w_hbm,
    list_hbm,
    out_ref,
    x_ref,
    s_ref,
    list_ref,
    in_sem,
    x_sem,
    w_sem,
    even_buf,
    odd_buf,
    pall,
    pbuf,
    lhs_buf,
    wbuf,
    own_buf,
    share_buf,
    merged_buf,
    near_buf,
    got_buf,
    pick_buf,
    acc_buf,
    psend,
    precv,
    wsend,
    wrecv,
    ssend,
    srecv,
    msend,
    mrecv,
    nsend,
    nrecv,
):
    cores, nx, lo, hi = plan.cores, plan.nx, plan.lo, plan.hi
    halves, pair, chunks = plan.halves, plan.pair, plan.chunks
    cols, width, block = plan.cols, plan.width, plan.block
    half = width // 2
    offsets = plan.offsets
    count = len(offsets)
    g = lax.axis_index("grp")
    s = lax.axis_index("sub")
    core, xi = lax.rem(g, cores), lax.div(g, cores)
    z, y = lax.div(s, lo), lax.rem(s, lo)
    zh, zl = lax.div(z, pair), lax.rem(z, pair)
    is_end = zh == zl
    is_mid = zh != zl

    def peer(dx, dy, dc):
        gg = lax.rem(xi + dx, nx) * cores + lax.rem(core + dc, cores)
        yy = lax.rem(y + dy, lo)
        return gg, yy

    def level(zz):
        return (g, zz * lo + y)

    def half_of(h):
        return zh if h == halves - 1 else 1 - zh

    def slot(o, dc):
        return dc * count + o

    def hops(o):
        return sum(1 for v in offsets[o] if v)

    plane = [(o, dc) for o in range(count) for dc in range(cores) if (o, dc) != (0, 0)]
    plane.sort(key=lambda item: -hops(item[0]))

    load_s = pltpu.make_async_copy(s_hbm, s_ref, in_sem.at[0])
    load_s.start()

    def x_copy(h, gg):
        start = (gg * hi + half_of(h) * pair) * lo * block * 2
        return pltpu.make_async_copy(
            x_hbm.at[pl.ds(pl.multiple_of(start, 16), plan.rows_h * 2), :], x_ref.at[h, gg], x_sem.at[h, gg]
        )

    def w_copy(c):
        return pltpu.make_async_copy(w_hbm.at[:, pl.ds(c * cols, cols)], wbuf.at[c, 0], w_sem.at[c])

    for gg in range(plan.grp):
        x_copy(0, gg).start()
    for c in range(chunks):
        w_copy(c).start()
    for gg in range(plan.grp):
        x_copy(1, gg).start()
    load_list = pltpu.make_async_copy(list_hbm, list_ref, in_sem.at[1])
    load_list.start()

    barrier = pltpu.get_barrier_semaphore()
    for o, dc in plane:
        gg, yy = peer(*offsets[o], dc)
        pl.semaphore_signal(barrier, inc=1, device_id=(gg, z * lo + yy), device_id_type=MESH)
    near = level(zh * pair + 1 - zl)
    far_mid = level((1 - zh) * pair + zh)
    far_end = level((1 - zh) * pair + 1 - zh)
    pl.semaphore_signal(barrier, inc=1, device_id=near, device_id_type=MESH)
    pl.semaphore_signal(barrier, inc=1, device_id=far_mid, device_id_type=MESH)

    @pl.when(is_mid)
    def _():
        pl.semaphore_signal(barrier, inc=1, device_id=far_end, device_id_type=MESH)

    load_s.wait()
    upper = s_ref[...]
    both = jnp.concatenate([upper, -upper[half:], upper[:half]], axis=0)
    contract = (((1,), (1,)), ((), ()))

    def partial(h):
        for gg in range(plan.grp):
            x_copy(h, gg).wait()
            value = lax.dot_general(x_ref[h, gg], both, contract, preferred_element_type=F32)
            b = gg % 2
            even_buf[b] = value[:, :width]
            odd_buf[b] = value[:, width:]
            value = (
                even_buf[b, pl.ds(0, plan.rows_h, stride=2), :] + odd_buf[b, pl.ds(1, plan.rows_h, stride=2), :]
            )
            pall[h, gg] = value.reshape(pair, lo, block, width).astype(BF16)

    sends = []

    def remote(src, dst, send, recv, target):
        return pltpu.make_async_remote_copy(
            src_ref=src, dst_ref=dst, send_sem=send, recv_sem=recv, device_id=target, device_id_type=MESH
        )

    def arrived(ref, sem):
        pltpu.make_async_copy(ref, ref, sem).wait()

    def wait_w(c, k):
        arrived(wbuf.at[c, k], wrecv.at[c, k])

    def send_w(c):
        w_copy(c).wait()
        for o in sorted(range(count), key=lambda o: -hops(o)):
            if o == 0 and cores == 1:
                continue
            dc = 1 if o == 0 else 0
            gg, yy = peer(*offsets[o], dc)
            k = slot(o, dc)
            copy = remote(wbuf.at[c, 0], wbuf.at[c, k], wsend.at[c, k], wrecv.at[c, k], (gg, z * lo + yy))
            copy.start()
            sends.append(copy)

    def relay_w(c):
        if cores == 1:
            return
        gg, yy = peer(0, 0, 1)
        for o in sorted(range(1, count), key=hops):
            wait_w(c, slot(o, 0))
            k = slot(o, 1)
            copy = remote(wbuf.at[c, slot(o, 0)], wbuf.at[c, k], wsend.at[c, k], wrecv.at[c, k], (gg, z * lo + yy))
            copy.start()
            sends.append(copy)

    def ready_w(c):
        for o in range(count):
            if cores > 1:
                wait_w(c, slot(o, 1))
            elif o > 0:
                wait_w(c, slot(o, 0))

    def send_p(h):
        for o, dc in plane:
            gg, yy = peer(*offsets[o], dc)
            k = slot(o, dc)
            copy = remote(pall.at[h, gg, :, yy], pbuf.at[h, k], psend.at[h, k], precv.at[h, k], (gg, z * lo + yy))
            copy.start()
            sends.append(copy)

    sign = jnp.where(lax.broadcasted_iota(jnp.int32, (block, width), 1) < half, 1.0, -1.0).astype(F32)

    def place(h, k, value):
        for p in range(pair):
            rows = value[p].astype(F32)
            columns = pl.ds(k * width, width)
            lhs_buf[h, pl.ds(2 * p * block, block), columns] = (rows * sign).astype(BF16)
            turned = jnp.concatenate([rows[:, half:], rows[:, :half]], axis=1)
            lhs_buf[h, pl.ds((2 * p + 1) * block, block), columns] = turned.astype(BF16)

    def wait_p(h):
        place(h, 0, pall[h, g, :, y])
        for o, dc in reversed(plane):
            k = slot(o, dc)
            arrived(pbuf.at[h, k], precv.at[h, k])
            place(h, k, pbuf[h, k])

    def product(h, c):
        weights = wbuf[c].reshape(plan.slots * width, cols)
        value = jnp.dot(lhs_buf[h], weights, preferred_element_type=F32).reshape(pair, 2, block, cols)
        own_buf[h, c] = value
        share_buf[h, c] = value.astype(BF16)

    def to_near(c):
        return remote(share_buf.at[0, c], near_buf.at[c], nsend.at[c], nrecv.at[c], near)

    def to_owner(c, p):
        return remote(
            merged_buf.at[c, p], got_buf.at[c, 1], msend.at[c, p], mrecv.at[c], level((1 - zh) * pair + p)
        )

    def first(c):
        product(0, c)

        @pl.when(is_end)
        def _():
            to_near(c).start()

    def merge(c):
        @pl.when(is_mid)
        def _():
            arrived(near_buf.at[c], nrecv.at[c])
            merged_buf[c] = (own_buf[0, c] + near_buf[c].astype(F32)).astype(BF16)
            for p in range(pair):
                to_owner(c, p).start()

    def second(c):
        product(1, c)
        copy = remote(share_buf.at[1, c, 1 - zl], got_buf.at[c, 0], ssend.at[c], srecv.at[c], near)
        copy.start()
        sends.append(copy)

    def finish(c):
        arrived(got_buf.at[c, 1], mrecv.at[c])
        total = own_buf[1, c, zl] + got_buf[c, 1].astype(F32)
        arrived(got_buf.at[c, 0], srecv.at[c])
        total = total + got_buf[c, 0].astype(F32)
        rounded = total.astype(BF16).reshape(2 * block, cols)
        placed = jnp.dot(rounded, pick_buf[pl.ds(c * cols, cols), :], preferred_element_type=F32)
        if c == 0:
            acc_buf[...] = placed
        elif c < chunks - 1:
            acc_buf[...] += placed
        else:
            out_ref[...] = (acc_buf[...] + placed).astype(BF16).reshape(2, block, plan.beams)

    partial(0)
    pl.semaphore_wait(barrier, len(plane) + jnp.where(is_mid, 3, 2))
    send_w(0)
    send_p(0)
    for c in range(1, min(AHEAD, chunks)):
        send_w(c)
    partial(1)
    load_list.wait()
    for c in range(chunks):
        row = lax.broadcasted_iota(jnp.int32, (cols, plan.beams), 0) + c * cols
        pick_buf[pl.ds(c * cols, cols), :] = jnp.where(row == list_ref[...], 1.0, 0.0).astype(BF16)
    relay_w(0)
    wait_p(0)
    for c in range(chunks):
        if c + AHEAD < chunks:
            send_w(c + AHEAD)
        if c == min(SECOND, chunks - 1):
            send_p(1)
        if c + 1 < chunks:
            relay_w(c + 1)
        ready_w(c)
        first(c)
        if c >= LAG:
            merge(c - LAG)
    wait_p(1)
    left = list(range(max(chunks - LAG, 0), chunks))
    for c in range(chunks):
        second(c)
        if c % 2 == 1 and left:
            merge(left.pop(0))
    for c in left:
        merge(c)
    for c in range(chunks):
        finish(c)

    for copy in sends:
        copy.wait_send()

    @pl.when(is_end)
    def _():
        for c in range(chunks):
            to_near(c).wait_send()

    @pl.when(is_mid)
    def _():
        for c in range(chunks):
            for p in range(pair):
                to_owner(c, p).wait_send()


def shards(plan, snapshots, steering, combining, beam_list):
    snap, _, _, elements = snapshots.shape
    signal = snapshots.reshape(snap * 2, elements)
    steer = jnp.transpose(steering[0], (0, 2, 1)).reshape(plan.width, elements)
    weights = combining.reshape(plan.width, plan.beams)
    pair, block, cols, chunks, halves = plan.pair, plan.block, plan.cols, plan.chunks, plan.halves
    hbm = pl.BlockSpec(memory_space=pl.ANY)
    dma = pltpu.SemaphoreType.DMA
    return pl.pallas_call(
        functools.partial(beam_kernel, plan),
        out_shape=jax.ShapeDtypeStruct((2, block, plan.beams), BF16),
        in_specs=[hbm, hbm, hbm, hbm],
        out_specs=pl.BlockSpec(memory_space=pltpu.VMEM),
        scratch_shapes=[
            pltpu.VMEM((halves, plan.grp, plan.rows_h * 2, elements), BF16),
            pltpu.VMEM((plan.width, elements), BF16),
            pltpu.VMEM((1, plan.beams), jnp.int32),
            dma((2,)),
            dma((halves, plan.grp)),
            dma((chunks,)),
            pltpu.VMEM((2, plan.rows_h * 2, plan.width), F32),
            pltpu.VMEM((2, plan.rows_h * 2, plan.width), F32),
            pltpu.VMEM((halves, plan.grp, pair, plan.lo, block, plan.width), BF16),
            pltpu.VMEM((halves, plan.slots, pair, block, plan.width), BF16),
            pltpu.VMEM((halves, pair * 2 * block, plan.slots * plan.width), BF16),
            pltpu.VMEM((chunks, plan.slots, plan.width, cols), BF16),
            pltpu.VMEM((halves, chunks, pair, 2, block, cols), F32),
            pltpu.VMEM((halves, chunks, pair, 2, block, cols), BF16),
            pltpu.VMEM((chunks, pair, 2, block, cols), BF16),
            pltpu.VMEM((chunks, pair, 2, block, cols), BF16),
            pltpu.VMEM((chunks, 2, 2, block, cols), BF16),
            pltpu.VMEM((plan.beams, plan.beams), BF16),
            pltpu.VMEM((2 * block, plan.beams), F32),
            dma((halves, plan.slots)),
            dma((halves, plan.slots)),
            dma((chunks, plan.slots)),
            dma((chunks, plan.slots)),
            dma((chunks,)),
            dma((chunks,)),
            dma((chunks, pair)),
            dma((chunks,)),
            dma((chunks,)),
            dma((chunks,)),
        ],
        compiler_params=pltpu.CompilerParams(
            collective_id=0, has_side_effects=True, vmem_limit_bytes=VMEM_LIMIT
        ),
    )(signal, steer, weights, beam_list.reshape(1, plan.beams))


def solution(mesh):
    placed = (
        P(None, None, ("grp", "sub"), None),
        P(("grp", "sub"), None, None, None),
        P(("grp", "sub"), None, None, None),
        P(),
    )

    def whole(snapshots, steering, combining, beam_list):
        plan = Plan(mesh, snapshots.shape[0], 2 * steering.shape[3], combining.shape[3])
        return jax.shard_map(
            functools.partial(shards, plan),
            mesh=mesh,
            in_specs=placed,
            out_specs=P(None, ("grp", "sub"), None),
            check_vma=False,
        )(snapshots, steering, combining, beam_list)

    return whole
```

```python
import functools

import jax
import jax.numpy as jnp
from jax import lax
from jax.experimental import pallas as pl
from jax.experimental.pallas import tpu as pltpu
from jax.sharding import PartitionSpec as P

MESH = pl.DeviceIdType.MESH
F32 = jnp.float32
BF16 = jnp.bfloat16
AHEAD = 4
PRE = 1
END = [
    "W4",
    "W5",
    "W6",
    "W7",
    "X",
    "R0",
    "P0",
    "Y0",
    "F0",
    "R1",
    "Y1",
    "F1",
    "R2",
    "Y2",
    "F2",
    "R3",
    "Y3",
    "F3",
    "R4",
    "Y4",
    "F4",
    "R5",
    "Y5",
    "F5",
    "R6",
    "Y6",
    "F6",
    "R7",
    "Y7",
    "F7",
    "P1",
    "S0",
    "S1",
    "S2",
    "S3",
    "S4",
    "S5",
    "S6",
    "S7",
]
MID = [
    "W4",
    "X",
    "W5",
    "W6",
    "W7",
    "R0",
    "P0",
    "Y0",
    "F0",
    "R1",
    "Y1",
    "F1",
    "R2",
    "Y2",
    "F2",
    "M0",
    "R3",
    "Y3",
    "F3",
    "M1",
    "R4",
    "Y4",
    "F4",
    "M2",
    "P1",
    "S0",
    "M3",
    "R5",
    "S1",
    "M4",
    "S2",
    "Y5",
    "F5",
    "R6",
    "S3",
    "M5",
    "S4",
    "Y6",
    "F6",
    "R7",
    "S5",
    "M6",
    "S6",
    "Y7",
    "F7",
    "S7",
    "M7",
]
VMEM_LIMIT = 60 * 1024 * 1024


class Plan:
    def __init__(self, mesh, snap, width, beams):
        self.grp = mesh.shape["grp"]
        self.sub = mesh.shape["sub"]
        self.cores = 2 if self.grp % 2 == 0 else 1
        self.nx = self.grp // self.cores
        self.halves, self.pair = 2, 2
        self.hi = self.halves * self.pair
        self.lo = self.sub // self.hi
        self.block = snap // (self.grp * self.sub)
        self.width = width
        self.beams = beams
        self.chunks = 8 if beams % 1024 == 0 else 1
        self.cols = beams // self.chunks
        self.offsets = [(dx, dy) for dx in range(self.nx) for dy in range(self.lo)]
        self.slots = len(self.offsets) * self.cores
        self.rows_h = self.pair * self.lo * self.block

    def steps(self, steps):
        if self.chunks == 8:
            return steps
        plain = [f"W{c}" for c in range(min(AHEAD, self.chunks), self.chunks)] + ["X", "R0", "P0", "Y0", "F0"]
        for c in range(1, self.chunks):
            plain += [f"R{c}", f"Y{c}", f"F{c}"]
        plain += [f"M{c}" for c in range(self.chunks) if "M0" in steps] + ["P1"]
        return plain + [f"S{c}" for c in range(self.chunks)]


def beam_kernel(
    plan,
    x_hbm,
    s_hbm,
    w_hbm,
    list_hbm,
    out_ref,
    x_ref,
    s_ref,
    both_buf,
    list_ref,
    in_sem,
    w_sem,
    even_buf,
    odd_buf,
    pall,
    pbuf,
    lhs_buf,
    wbuf,
    own_buf,
    share_buf,
    pass_buf,
    last_buf,
    near_buf,
    got_buf,
    pick_buf,
    acc_buf,
    send_sem,
    precv,
    wrecv,
    srecv,
    mrecv,
    nrecv,
):
    cores, nx, lo, hi = plan.cores, plan.nx, plan.lo, plan.hi
    halves, pair, chunks = plan.halves, plan.pair, plan.chunks
    cols, width, block = plan.cols, plan.width, plan.block
    half = width // 2
    offsets = plan.offsets
    count = len(offsets)
    g = lax.axis_index("grp")
    s = lax.axis_index("sub")
    core, xi = lax.rem(g, cores), lax.div(g, cores)
    z, y = lax.div(s, lo), lax.rem(s, lo)
    zh, zl = lax.div(z, pair), lax.rem(z, pair)
    is_end = zh == zl
    is_mid = zh != zl

    def peer(dx, dy, dc):
        gg = lax.rem(xi + dx, nx) * cores + lax.rem(core + dc, cores)
        yy = lax.rem(y + dy, lo)
        return gg, yy

    def level(zz):
        return (g, zz * lo + y)

    def half_of(h):
        return zh if h == halves - 1 else 1 - zh

    def slot(o, dc):
        return dc * count + o

    def hops(o):
        return sum(1 for v in offsets[o] if v)

    plane = [(o, dc) for o in range(count) for dc in range(cores) if (o, dc) != (0, 0)]
    plane.sort(key=lambda item: -hops(item[0]))

    barrier = pltpu.get_barrier_semaphore()
    for o, dc in plane:
        gg, yy = peer(*offsets[o], dc)
        pl.semaphore_signal(barrier, inc=1, device_id=(gg, z * lo + yy), device_id_type=MESH)
    near = level(zh * pair + 1 - zl)
    far_mid = level((1 - zh) * pair + zh)
    far_end = level((1 - zh) * pair + 1 - zh)
    pl.semaphore_signal(barrier, inc=1, device_id=near, device_id_type=MESH)
    pl.semaphore_signal(barrier, inc=1, device_id=far_mid, device_id_type=MESH)

    @pl.when(is_mid)
    def _():
        pl.semaphore_signal(barrier, inc=1, device_id=far_end, device_id_type=MESH)

    load_s = pltpu.make_async_copy(s_hbm, s_ref, in_sem.at[0])

    def x_copy(h, gg):
        start = (gg * hi + half_of(h) * pair) * lo * block * 2
        return pltpu.make_async_copy(
            x_hbm.at[pl.ds(pl.multiple_of(start, 16), plan.rows_h * 2), :], x_ref.at[h, gg], in_sem.at[2 + h]
        )

    def w_copy(c):
        return pltpu.make_async_copy(w_hbm.at[:, pl.ds(c * cols, cols)], wbuf.at[c, 0], w_sem.at[c])

    w_copy(0).start()
    load_s.start()
    for gg in range(plan.grp):
        x_copy(0, gg).start()
    for c in range(1, chunks):
        w_copy(c).start()
    for gg in range(plan.grp):
        x_copy(1, gg).start()
    load_list = pltpu.make_async_copy(list_hbm, list_ref, in_sem.at[1])
    load_list.start()

    contract = (((1,), (1,)), ((), ()))

    def stack():
        load_s.wait()
        upper = s_ref[...]
        both_buf[...] = jnp.concatenate([upper, -upper[half:], upper[:half]], axis=0)

    def partial(h):
        both = both_buf[...]
        arrived(x_ref.at[h], in_sem.at[2 + h])
        for gg in range(plan.grp):
            value = lax.dot_general(x_ref[h, gg], both, contract, preferred_element_type=F32)
            b = gg % 2
            even_buf[b] = value[:, :width]
            odd_buf[b] = value[:, width:]
            value = (
                even_buf[b, pl.ds(0, plan.rows_h, stride=2), :] + odd_buf[b, pl.ds(1, plan.rows_h, stride=2), :]
            )
            pall[h, gg] = value.reshape(pair, lo, block, width).astype(BF16)

    def remote(src, dst, send, recv, target):
        return pltpu.make_async_remote_copy(
            src_ref=src, dst_ref=dst, send_sem=send, recv_sem=recv, device_id=target, device_id_type=MESH
        )

    def arrived(ref, sem):
        pltpu.make_async_copy(ref, ref, sem).wait()

    def send_w(c):
        w_copy(c).wait()
        for o in sorted(range(count), key=lambda o: -hops(o)):
            if o == 0 and cores == 1:
                continue
            dc = cores - 1
            gg, yy = peer(*offsets[o], dc)
            k = slot(o, dc)
            sem = wrecv.at[c, 1 if o == 0 else 0]
            remote(wbuf.at[c, 0], wbuf.at[c, k], send_sem.at[0], sem, (gg, z * lo + yy)).start()

    def relay_w(c):
        arrived(wbuf.at[c, pl.ds(slot(1, cores - 1), count - 1)], wrecv.at[c, 0])
        if cores == 1:
            return
        gg, yy = peer(0, 0, 1)
        for o in range(1, count):
            source = wbuf.at[c, slot(o, 1)]
            remote(source, wbuf.at[c, o], send_sem.at[0], wrecv.at[c, 1], (gg, z * lo + yy)).start()

    def ready_w(c):
        if cores > 1:
            arrived(wbuf.at[c, pl.ds(1, count)], wrecv.at[c, 1])

    def send_p(h):
        for o, dc in plane:
            gg, yy = peer(*offsets[o], dc)
            k = slot(o, dc)
            source = pall.at[h, gg, :, yy]
            remote(source, pbuf.at[h, k], send_sem.at[1], precv.at[h], (gg, z * lo + yy)).start()

    sign = jnp.where(lax.broadcasted_iota(jnp.int32, (block, width), 1) < half, 1.0, -1.0).astype(F32)
    orders = ((1 - zh, zh), (1 - zl, zl))

    def place(h, k, rows):
        for i in range(pair):
            row = (h * pair + i) * 2 * block
            part = rows(i).astype(F32)
            columns = pl.ds(k * width, width)
            lhs_buf[pl.ds(row, block), columns] = (part * sign).astype(BF16)
            turned = jnp.concatenate([part[:, half:], part[:, :half]], axis=1)
            lhs_buf[pl.ds(row + block, block), columns] = turned.astype(BF16)

    def wait_p(h):
        place(h, 0, lambda i: pall[h, g, orders[h][i], y])
        arrived(pbuf.at[h, pl.ds(1, plan.slots - 1)], precv.at[h])
        for o, dc in plane:
            k = slot(o, dc)
            place(h, k, lambda i: pbuf[h, k, orders[h][i]])

    def product(h, c):
        weights = wbuf[c].reshape(plan.slots * width, cols)
        left = lhs_buf[pl.ds(h * pair * 2 * block, pair * 2 * block), :]
        return jnp.dot(left, weights, preferred_element_type=F32).reshape(pair, 2, block, cols)

    def to_near(c, i):
        return remote(share_buf.at[c, i], near_buf.at[c, i], send_sem.at[2], nrecv.at[c, i], near)

    def to_owner(c, i):
        target = level((1 - zh) * pair + orders[0][i])
        return remote(share_buf.at[c, i], got_buf.at[c, 1], send_sem.at[2], mrecv.at[c], target)

    def to_pair(c):
        return remote(pass_buf.at[c], got_buf.at[c, 0], send_sem.at[3], srecv.at[c], near)

    def first_end(c):
        share_buf[c] = product(0, c).astype(BF16)
        for i in range(pair):
            to_near(c, i).start()

    def first_mid(c):
        own_buf[c] = product(0, c)

    def merge(c):
        for i in range(pair):
            arrived(near_buf.at[c, i], nrecv.at[c, i])
            share_buf[c, i] = (own_buf[c, i] + near_buf[c, i].astype(F32)).astype(BF16)
            to_owner(c, i).start()

    def second(c):
        value = product(1, c)
        pass_buf[c] = value[0].astype(BF16)
        to_pair(c).start()
        last_buf[c] = value[1]

    def finish(c):
        arrived(got_buf.at[c, 1], mrecv.at[c])
        total = last_buf[c] + got_buf[c, 1].astype(F32)
        arrived(got_buf.at[c, 0], srecv.at[c])
        total = total + got_buf[c, 0].astype(F32)
        rounded = total.astype(BF16).reshape(2 * block, cols)
        placed = jnp.dot(rounded, pick_buf[pl.ds(c * cols, cols), :], preferred_element_type=F32)
        if c == 0:
            acc_buf[...] = placed
        elif c < chunks - 1:
            acc_buf[...] += placed
        else:
            out_ref[...] = (acc_buf[...] + placed).astype(BF16).reshape(2, block, plan.beams)

    pl.semaphore_wait(barrier, len(plane) + jnp.where(is_mid, 3, 2))
    for c in range(min(PRE, chunks)):
        send_w(c)
    stack()
    partial(0)
    send_p(0)
    for c in range(min(PRE, chunks), min(AHEAD, chunks)):
        send_w(c)
    partial(1)
    load_list.wait()
    for c in range(chunks):
        row = lax.broadcasted_iota(jnp.int32, (cols, plan.beams), 0) + c * cols
        pick_buf[pl.ds(c * cols, cols), :] = jnp.where(row == list_ref[...], 1.0, 0.0).astype(BF16)
    actions = {
        "W": send_w,
        "R": relay_w,
        "Y": ready_w,
        "M": merge,
        "P": wait_p,
        "S": second,
    }

    def follow(steps, first):
        for step in steps:
            if step == "X":
                send_p(1)
            elif step[0] == "F":
                first(int(step[1:]))
            else:
                actions[step[0]](int(step[1:]))

    @pl.when(is_end)
    def _():
        follow(plan.steps(END), first_end)

    @pl.when(is_mid)
    def _():
        follow(plan.steps(MID), first_mid)

    arrived(wbuf.at[:, pl.ds(1, plan.slots - 1)], send_sem.at[0])
    arrived(pbuf.at[:, pl.ds(1, plan.slots - 1)], send_sem.at[1])
    for c in range(chunks):
        if c == chunks - 1:
            arrived(share_buf, send_sem.at[2])
            arrived(pass_buf, send_sem.at[3])
        finish(c)


def shards(plan, snapshots, steering, combining, beam_list):
    snap, _, _, elements = snapshots.shape
    signal = snapshots.reshape(snap * 2, elements)
    steer = jnp.transpose(steering[0], (0, 2, 1)).reshape(plan.width, elements)
    weights = combining.reshape(plan.width, plan.beams)
    pair, block, cols, chunks, halves = plan.pair, plan.block, plan.cols, plan.chunks, plan.halves
    hbm = pl.BlockSpec(memory_space=pl.ANY)
    dma = pltpu.SemaphoreType.DMA
    return pl.pallas_call(
        functools.partial(beam_kernel, plan),
        out_shape=pltpu.VMEM((2, block, plan.beams), BF16),
        in_specs=[hbm, hbm, hbm, hbm],
        out_specs=pl.BlockSpec(memory_space=pltpu.VMEM),
        scratch_shapes=[
            pltpu.VMEM((halves, plan.grp, plan.rows_h * 2, elements), BF16),
            pltpu.VMEM((plan.width, elements), BF16),
            pltpu.VMEM((2 * plan.width, elements), BF16),
            pltpu.VMEM((1, plan.beams), jnp.int32),
            dma((2 + halves,)),
            dma((chunks,)),
            pltpu.VMEM((2, plan.rows_h * 2, plan.width), F32),
            pltpu.VMEM((2, plan.rows_h * 2, plan.width), F32),
            pltpu.VMEM((halves, plan.grp, pair, plan.lo, block, plan.width), BF16),
            pltpu.VMEM((halves, plan.slots, pair, block, plan.width), BF16),
            pltpu.VMEM((halves * pair * 2 * block, plan.slots * plan.width), BF16),
            pltpu.VMEM((chunks, plan.slots, plan.width, cols), BF16),
            pltpu.VMEM((chunks, pair, 2, block, cols), F32),
            pltpu.VMEM((chunks, pair, 2, block, cols), BF16),
            pltpu.VMEM((chunks, 2, block, cols), BF16),
            pltpu.VMEM((chunks, 2, block, cols), F32),
            pltpu.VMEM((chunks, pair, 2, block, cols), BF16),
            pltpu.VMEM((chunks, 2, 2, block, cols), BF16),
            pltpu.VMEM((plan.beams, plan.beams), BF16),
            pltpu.VMEM((2 * block, plan.beams), F32),
            dma((4,)),
            dma((halves,)),
            dma((chunks, 2)),
            dma((chunks,)),
            dma((chunks,)),
            dma((chunks, pair)),
        ],
        compiler_params=pltpu.CompilerParams(
            collective_id=0, has_side_effects=True, vmem_limit_bytes=VMEM_LIMIT
        ),
    )(signal, steer, weights, beam_list.reshape(1, plan.beams))


def solution(mesh):
    placed = (
        P(None, None, ("grp", "sub"), None),
        P(("grp", "sub"), None, None, None),
        P(("grp", "sub"), None, None, None),
        P(),
    )

    def whole(snapshots, steering, combining, beam_list):
        plan = Plan(mesh, snapshots.shape[0], 2 * steering.shape[3], combining.shape[3])
        return jax.shard_map(
            functools.partial(shards, plan),
            mesh=mesh,
            in_specs=placed,
            out_specs=P(None, ("grp", "sub"), None),
            check_vma=False,
        )(snapshots, steering, combining, beam_list)

    return whole
```

```python
import functools

import jax
import jax.numpy as jnp
from jax import lax
from jax.experimental import pallas as pl
from jax.experimental.pallas import tpu as pltpu
from jax.sharding import PartitionSpec as P

MESH = pl.DeviceIdType.MESH
F32 = jnp.float32
BF16 = jnp.bfloat16
AHEAD = 4
PRE = 1
END = [
    "W4",
    "W5",
    "W6",
    "W7",
    "X",
    "R0",
    "P0",
    "Y0",
    "F0",
    "R1",
    "Y1",
    "F1",
    "R2",
    "Y2",
    "F2",
    "R3",
    "Y3",
    "F3",
    "R4",
    "Y4",
    "F4",
    "R5",
    "Y5",
    "F5",
    "R6",
    "Y6",
    "F6",
    "R7",
    "Y7",
    "F7",
    "P1",
    "S0",
    "S1",
    "S2",
    "S3",
    "S4",
    "S5",
    "S6",
    "S7",
]
MID = [
    "W4",
    "X",
    "W5",
    "W6",
    "W7",
    "R0",
    "P0",
    "Y0",
    "F0",
    "R1",
    "Y1",
    "F1",
    "M0",
    "R2",
    "Y2",
    "F2",
    "R3",
    "M1",
    "Y3",
    "F3",
    "R4",
    "M2",
    "Y4",
    "F4",
    "P1",
    "S0",
    "S1",
    "M3",
    "R5",
    "S2",
    "S3",
    "M4",
    "Y5",
    "F5",
    "R6",
    "S4",
    "M5",
    "Y6",
    "F6",
    "R7",
    "S5",
    "S6",
    "M6",
    "Y7",
    "F7",
    "M7",
    "S7",
]
VMEM_LIMIT = 60 * 1024 * 1024


class Plan:
    def __init__(self, mesh, snap, width, beams):
        self.grp = mesh.shape["grp"]
        self.sub = mesh.shape["sub"]
        self.cores = 2 if self.grp % 2 == 0 else 1
        self.nx = self.grp // self.cores
        self.halves, self.pair = 2, 2
        self.hi = self.halves * self.pair
        self.lo = self.sub // self.hi
        self.block = snap // (self.grp * self.sub)
        self.width = width
        self.beams = beams
        self.chunks = 8 if beams % 1024 == 0 else 1
        self.cols = beams // self.chunks
        self.offsets = [(dx, dy) for dx in range(self.nx) for dy in range(self.lo)]
        self.slots = len(self.offsets) * self.cores
        self.rows_h = self.pair * self.lo * self.block

    def steps(self, steps):
        if self.chunks == 8:
            return steps
        plain = [f"W{c}" for c in range(min(AHEAD, self.chunks), self.chunks)] + ["X", "R0", "P0", "Y0", "F0"]
        for c in range(1, self.chunks):
            plain += [f"R{c}", f"Y{c}", f"F{c}"]
        plain += [f"M{c}" for c in range(self.chunks) if "M0" in steps] + ["P1"]
        return plain + [f"S{c}" for c in range(self.chunks)]


def beam_kernel(
    plan,
    x_hbm,
    s_hbm,
    w_hbm,
    list_hbm,
    out_ref,
    x_ref,
    s_ref,
    both_buf,
    list_ref,
    in_sem,
    list_sem,
    even_buf,
    odd_buf,
    pall,
    pbuf,
    lhs_buf,
    wbuf,
    own_buf,
    share_buf,
    pass_buf,
    last_buf,
    near_buf,
    got_buf,
    pick_buf,
    acc_buf,
    send_sem,
    precv,
    wrecv,
    srecv,
    nrecv,
):
    cores, nx, lo, hi = plan.cores, plan.nx, plan.lo, plan.hi
    halves, pair, chunks = plan.halves, plan.pair, plan.chunks
    cols, width, block = plan.cols, plan.width, plan.block
    half = width // 2
    offsets = plan.offsets
    count = len(offsets)
    g = lax.axis_index("grp")
    s = lax.axis_index("sub")
    core, xi = lax.rem(g, cores), lax.div(g, cores)
    z, y = lax.div(s, lo), lax.rem(s, lo)
    zh, zl = lax.div(z, pair), lax.rem(z, pair)
    is_end = zh == zl
    is_mid = zh != zl

    def peer(dx, dy, dc):
        gg = lax.rem(xi + dx, nx) * cores + lax.rem(core + dc, cores)
        yy = lax.rem(y + dy, lo)
        return gg, yy

    def level(zz):
        return (g, zz * lo + y)

    def half_of(h):
        return zh if h == halves - 1 else 1 - zh

    def slot(o, dc):
        return dc * count + o

    def hops(o):
        return sum(1 for v in offsets[o] if v)

    plane = [(o, dc) for o in range(count) for dc in range(cores) if (o, dc) != (0, 0)]
    plane.sort(key=lambda item: -hops(item[0]))

    barrier = pltpu.get_barrier_semaphore()
    for o, dc in plane:
        gg, yy = peer(*offsets[o], dc)
        pl.semaphore_signal(barrier, inc=1, device_id=(gg, z * lo + yy), device_id_type=MESH)
    near = level(zh * pair + 1 - zl)
    far_mid = level((1 - zh) * pair + zh)
    far_end = level((1 - zh) * pair + 1 - zh)
    pl.semaphore_signal(barrier, inc=1, device_id=near, device_id_type=MESH)
    pl.semaphore_signal(barrier, inc=1, device_id=far_mid, device_id_type=MESH)

    @pl.when(is_mid)
    def _():
        pl.semaphore_signal(barrier, inc=1, device_id=far_end, device_id_type=MESH)

    load_s = pltpu.make_async_copy(s_hbm, s_ref, in_sem.at[0])

    def x_copy(h, gg):
        start = (gg * hi + half_of(h) * pair) * lo * block * 2
        return pltpu.make_async_copy(
            x_hbm.at[pl.ds(pl.multiple_of(start, 16), plan.rows_h * 2), :], x_ref.at[h, gg], in_sem.at[2 + h]
        )

    def w_copy(c):
        return pltpu.make_async_copy(w_hbm.at[:, pl.ds(c * cols, cols)], wbuf.at[c, 0], in_sem.at[4 if c else 1])

    w_copy(0).start()
    load_s.start()
    for gg in range(plan.grp):
        x_copy(0, gg).start()
    for c in range(1, chunks):
        w_copy(c).start()
    for gg in range(plan.grp):
        x_copy(1, gg).start()
    load_list = pltpu.make_async_copy(list_hbm, list_ref, list_sem)
    load_list.start()

    contract = (((1,), (1,)), ((), ()))

    def stack():
        load_s.wait()
        upper = s_ref[...]
        both_buf[...] = jnp.concatenate([upper, -upper[half:], upper[:half]], axis=0)

    def partial(h):
        both = both_buf[...]
        arrived(x_ref.at[h], in_sem.at[2 + h])
        for gg in range(plan.grp):
            value = lax.dot_general(x_ref[h, gg], both, contract, preferred_element_type=F32)
            b = gg % 2
            even_buf[b] = value[:, :width]
            odd_buf[b] = value[:, width:]
            value = (
                even_buf[b, pl.ds(0, plan.rows_h, stride=2), :] + odd_buf[b, pl.ds(1, plan.rows_h, stride=2), :]
            )
            pall[h, gg] = value.reshape(pair, lo, block, width).astype(BF16)

    def remote(src, dst, send, recv, target):
        return pltpu.make_async_remote_copy(
            src_ref=src, dst_ref=dst, send_sem=send, recv_sem=recv, device_id=target, device_id_type=MESH
        )

    def arrived(ref, sem):
        pltpu.make_async_copy(ref, ref, sem).wait()

    def send_w(c):
        if c == 0:
            w_copy(0).wait()
        if c == 1:
            arrived(wbuf.at[pl.ds(1, chunks - 1), 0], in_sem.at[4])
        for o in sorted(range(count), key=lambda o: -hops(o)):
            if o == 0 and cores == 1:
                continue
            dc = cores - 1
            gg, yy = peer(*offsets[o], dc)
            k = slot(o, dc)
            sem = wrecv.at[c, 1 if o == 0 else 0]
            remote(wbuf.at[c, 0], wbuf.at[c, k], send_sem.at[0], sem, (gg, z * lo + yy)).start()

    def relay_w(c):
        arrived(wbuf.at[c, pl.ds(slot(1, cores - 1), count - 1)], wrecv.at[c, 0])
        if cores == 1:
            return
        gg, yy = peer(0, 0, 1)
        for o in range(1, count):
            source = wbuf.at[c, slot(o, 1)]
            remote(source, wbuf.at[c, o], send_sem.at[0], wrecv.at[c, 1], (gg, z * lo + yy)).start()

    def ready_w(c):
        if cores > 1:
            arrived(wbuf.at[c, pl.ds(1, count)], wrecv.at[c, 1])

    def send_p(h):
        for o, dc in plane:
            gg, yy = peer(*offsets[o], dc)
            k = slot(o, dc)
            source = pall.at[h, gg, :, yy]
            remote(source, pbuf.at[h, k], send_sem.at[1], precv.at[h], (gg, z * lo + yy)).start()

    sign = jnp.where(lax.broadcasted_iota(jnp.int32, (block, width), 1) < half, 1.0, -1.0).astype(F32)
    orders = ((1 - zh, zh), (1 - zl, zl))

    def place(h, k, rows):
        for i in range(pair):
            row = (h * pair + i) * 2 * block
            part = rows(i).astype(F32)
            columns = pl.ds(k * width, width)
            lhs_buf[pl.ds(row, block), columns] = (part * sign).astype(BF16)
            turned = jnp.concatenate([part[:, half:], part[:, :half]], axis=1)
            lhs_buf[pl.ds(row + block, block), columns] = turned.astype(BF16)

    def wait_p(h):
        place(h, 0, lambda i: pall[h, g, orders[h][i], y])
        arrived(pbuf.at[h, pl.ds(1, plan.slots - 1)], precv.at[h])
        for o, dc in plane:
            k = slot(o, dc)
            place(h, k, lambda i: pbuf[h, k, orders[h][i]])

    def product(h, c):
        weights = wbuf[c].reshape(plan.slots * width, cols)
        left = lhs_buf[pl.ds(h * pair * 2 * block, pair * 2 * block), :]
        return jnp.dot(left, weights, preferred_element_type=F32).reshape(pair, 2, block, cols)

    def to_near(c, i):
        return remote(share_buf.at[c, i], near_buf.at[c, i], send_sem.at[2], nrecv.at[c + i if c == chunks - 1 else c], near)

    def to_owner(c, i):
        target = level((1 - zh) * pair + orders[0][i])
        return remote(share_buf.at[c, i], got_buf.at[c, 1], send_sem.at[2], srecv.at[c], target)

    def to_pair(c):
        return remote(pass_buf.at[c], got_buf.at[c, 0], send_sem.at[3], srecv.at[c], near)

    def first_end(c):
        share_buf[c] = product(0, c).astype(BF16)
        for i in range(pair):
            to_near(c, i).start()

    def first_mid(c):
        own_buf[c] = product(0, c)

    def merge(c):
        if c < chunks - 1:
            arrived(near_buf.at[c], nrecv.at[c])
        for i in range(pair):
            if c == chunks - 1:
                arrived(near_buf.at[c, i], nrecv.at[c + i])
            share_buf[c, i] = (own_buf[c, i] + near_buf[c, i].astype(F32)).astype(BF16)
            to_owner(c, i).start()

    def second(c):
        value = product(1, c)
        pass_buf[c] = value[0].astype(BF16)
        to_pair(c).start()
        last_buf[c] = value[1]

    def finish(c):
        arrived(got_buf.at[c], srecv.at[c])
        total = last_buf[c] + got_buf[c, 1].astype(F32) + got_buf[c, 0].astype(F32)
        rounded = total.astype(BF16).reshape(2 * block, cols)
        placed = jnp.dot(rounded, pick_buf[pl.ds(c * cols, cols), :], preferred_element_type=F32)
        if c == 0:
            acc_buf[...] = placed
        elif c < chunks - 1:
            acc_buf[...] += placed
        else:
            out_ref[...] = (acc_buf[...] + placed).astype(BF16).reshape(2, block, plan.beams)

    pl.semaphore_wait(barrier, len(plane) + jnp.where(is_mid, 3, 2))
    for c in range(min(PRE, chunks)):
        send_w(c)
    stack()
    partial(0)
    send_p(0)
    for c in range(min(PRE, chunks), min(AHEAD, chunks)):
        send_w(c)
    partial(1)
    load_list.wait()
    for c in range(chunks):
        row = lax.broadcasted_iota(jnp.int32, (cols, plan.beams), 0) + c * cols
        pick_buf[pl.ds(c * cols, cols), :] = jnp.where(row == list_ref[...], 1.0, 0.0).astype(BF16)
    actions = {
        "W": send_w,
        "R": relay_w,
        "Y": ready_w,
        "M": merge,
        "P": wait_p,
        "S": second,
    }

    def follow(steps, first):
        for step in steps:
            if step == "X":
                send_p(1)
            elif step[0] == "F":
                first(int(step[1:]))
            else:
                actions[step[0]](int(step[1:]))

    @pl.when(is_end)
    def _():
        follow(plan.steps(END), first_end)

    @pl.when(is_mid)
    def _():
        follow(plan.steps(MID), first_mid)

    arrived(wbuf.at[:, pl.ds(1, plan.slots - 1)], send_sem.at[0])
    arrived(pbuf.at[:, pl.ds(1, plan.slots - 1)], send_sem.at[1])
    for c in range(chunks):
        if c == chunks - 1:
            arrived(share_buf, send_sem.at[2])
            arrived(pass_buf, send_sem.at[3])
        finish(c)


def shards(plan, snapshots, steering, combining, beam_list):
    snap, _, _, elements = snapshots.shape
    signal = snapshots.reshape(snap * 2, elements)
    steer = jnp.transpose(steering[0], (0, 2, 1)).reshape(plan.width, elements)
    weights = combining.reshape(plan.width, plan.beams)
    pair, block, cols, chunks, halves = plan.pair, plan.block, plan.cols, plan.chunks, plan.halves
    hbm = pl.BlockSpec(memory_space=pl.ANY)
    dma = pltpu.SemaphoreType.DMA
    return pl.pallas_call(
        functools.partial(beam_kernel, plan),
        out_shape=pltpu.VMEM((2, block, plan.beams), BF16),
        in_specs=[hbm, hbm, hbm, hbm],
        out_specs=pl.BlockSpec(memory_space=pltpu.VMEM),
        scratch_shapes=[
            pltpu.VMEM((halves, plan.grp, plan.rows_h * 2, elements), BF16),
            pltpu.VMEM((plan.width, elements), BF16),
            pltpu.VMEM((2 * plan.width, elements), BF16),
            pltpu.VMEM((1, plan.beams), jnp.int32),
            dma((5,)),
            dma(()),
            pltpu.VMEM((2, plan.rows_h * 2, plan.width), F32),
            pltpu.VMEM((2, plan.rows_h * 2, plan.width), F32),
            pltpu.VMEM((halves, plan.grp, pair, plan.lo, block, plan.width), BF16),
            pltpu.VMEM((halves, plan.slots, pair, block, plan.width), BF16),
            pltpu.VMEM((halves * pair * 2 * block, plan.slots * plan.width), BF16),
            pltpu.VMEM((chunks, plan.slots, plan.width, cols), BF16),
            pltpu.VMEM((chunks, pair, 2, block, cols), F32),
            pltpu.VMEM((chunks, pair, 2, block, cols), BF16),
            pltpu.VMEM((chunks, 2, block, cols), BF16),
            pltpu.VMEM((chunks, 2, block, cols), F32),
            pltpu.VMEM((chunks, pair, 2, block, cols), BF16),
            pltpu.VMEM((chunks, 2, 2, block, cols), BF16),
            pltpu.VMEM((plan.beams, plan.beams), BF16),
            pltpu.VMEM((2 * block, plan.beams), F32),
            dma((4,)),
            dma((halves,)),
            dma((chunks, 2)),
            dma((chunks,)),
            dma((chunks + 1,)),
        ],
        compiler_params=pltpu.CompilerParams(
            collective_id=0, has_side_effects=True, vmem_limit_bytes=VMEM_LIMIT
        ),
    )(signal, steer, weights, beam_list.reshape(1, plan.beams))


def solution(mesh):
    placed = (
        P(None, None, ("grp", "sub"), None),
        P(("grp", "sub"), None, None, None),
        P(("grp", "sub"), None, None, None),
        P(),
    )

    def whole(snapshots, steering, combining, beam_list):
        plan = Plan(mesh, snapshots.shape[0], 2 * steering.shape[3], combining.shape[3])
        return jax.shard_map(
            functools.partial(shards, plan),
            mesh=mesh,
            in_specs=placed,
            out_specs=P(None, ("grp", "sub"), None),
            check_vma=False,
        )(snapshots, steering, combining, beam_list)

    return whole
```

```python
import functools

import jax
import jax.numpy as jnp
from jax import lax
from jax.experimental import pallas as pl
from jax.experimental.pallas import tpu as pltpu
from jax.sharding import PartitionSpec as P

MESH = pl.DeviceIdType.MESH
F32 = jnp.float32
BF16 = jnp.bfloat16
AHEAD = 4
PRE = 1
END = [
    "W4",
    "W5",
    "W6",
    "W7",
    "X",
    "R0",
    "P0",
    "Y0",
    "F0",
    "R1",
    "Y1",
    "F1",
    "R2",
    "Y2",
    "F2",
    "R3",
    "Y3",
    "F3",
    "R4",
    "Y4",
    "F4",
    "R5",
    "Y5",
    "F5",
    "R6",
    "Y6",
    "F6",
    "R7",
    "Y7",
    "F7",
    "P1",
    "S0",
    "S1",
    "S2",
    "S3",
    "S4",
    "S5",
    "S6",
    "S7",
]
MID = [
    "W4",
    "X",
    "W5",
    "W6",
    "W7",
    "R0",
    "P0",
    "Y0",
    "F0",
    "R1",
    "Y1",
    "F1",
    "M0",
    "R2",
    "Y2",
    "F2",
    "R3",
    "M1",
    "Y3",
    "F3",
    "R4",
    "M2",
    "Y4",
    "F4",
    "P1",
    "S0",
    "S1",
    "M3",
    "R5",
    "S2",
    "S3",
    "M4",
    "Y5",
    "F5",
    "R6",
    "S4",
    "M5",
    "Y6",
    "F6",
    "R7",
    "S5",
    "S6",
    "M6",
    "Y7",
    "F7",
    "M7",
    "S7",
]
VMEM_LIMIT = 60 * 1024 * 1024


class Plan:
    def __init__(self, mesh, snap, width, beams):
        self.grp = mesh.shape["grp"]
        self.sub = mesh.shape["sub"]
        self.cores = 2 if self.grp % 2 == 0 else 1
        self.nx = self.grp // self.cores
        self.halves, self.pair = 2, 2
        self.hi = self.halves * self.pair
        self.lo = self.sub // self.hi
        self.block = snap // (self.grp * self.sub)
        self.width = width
        self.beams = beams
        self.chunks = 8 if beams % 1024 == 0 else 1
        self.cols = beams // self.chunks
        self.offsets = [(dx, dy) for dx in range(self.nx) for dy in range(self.lo)]
        self.slots = len(self.offsets) * self.cores
        self.rows_h = self.pair * self.lo * self.block

    def steps(self, steps):
        if self.chunks == 8:
            return steps
        plain = [f"W{c}" for c in range(min(AHEAD, self.chunks), self.chunks)] + ["X", "R0", "P0", "Y0", "F0"]
        for c in range(1, self.chunks):
            plain += [f"R{c}", f"Y{c}", f"F{c}"]
        plain += [f"M{c}" for c in range(self.chunks) if "M0" in steps] + ["P1"]
        return plain + [f"S{c}" for c in range(self.chunks)]


def beam_kernel(
    plan,
    x_hbm,
    s_hbm,
    w_hbm,
    list_hbm,
    out_ref,
    x_ref,
    s_ref,
    both_buf,
    list_ref,
    in_sem,
    list_sem,
    even_buf,
    odd_buf,
    pall,
    pbuf,
    lhs_buf,
    wbuf,
    own_buf,
    share_buf,
    pass_buf,
    last_buf,
    near_buf,
    got_buf,
    pick_buf,
    acc_buf,
    send_sem,
    precv,
    wrecv,
    srecv,
    nrecv,
):
    cores, nx, lo, hi = plan.cores, plan.nx, plan.lo, plan.hi
    halves, pair, chunks = plan.halves, plan.pair, plan.chunks
    cols, width, block = plan.cols, plan.width, plan.block
    half = width // 2
    offsets = plan.offsets
    count = len(offsets)
    g = lax.axis_index("grp")
    s = lax.axis_index("sub")
    core, xi = lax.rem(g, cores), lax.div(g, cores)
    z, y = lax.div(s, lo), lax.rem(s, lo)
    zh, zl = lax.div(z, pair), lax.rem(z, pair)
    is_end = zh == zl
    is_mid = zh != zl

    def peer(dx, dy, dc):
        gg = lax.rem(xi + dx, nx) * cores + lax.rem(core + dc, cores)
        yy = lax.rem(y + dy, lo)
        return gg, yy

    def level(zz):
        return (g, zz * lo + y)

    def half_of(h):
        return zh if h == halves - 1 else 1 - zh

    def slot(o, dc):
        return dc * count + o

    def hops(o):
        return sum(1 for v in offsets[o] if v)

    plane = [(o, dc) for o in range(count) for dc in range(cores) if (o, dc) != (0, 0)]
    plane.sort(key=lambda item: -hops(item[0]))

    barrier = pltpu.get_barrier_semaphore()
    for o, dc in plane:
        gg, yy = peer(*offsets[o], dc)
        pl.semaphore_signal(barrier, inc=1, device_id=(gg, z * lo + yy), device_id_type=MESH)
    near = level(zh * pair + 1 - zl)
    far_mid = level((1 - zh) * pair + zh)
    far_end = level((1 - zh) * pair + 1 - zh)
    pl.semaphore_signal(barrier, inc=1, device_id=near, device_id_type=MESH)
    pl.semaphore_signal(barrier, inc=1, device_id=far_mid, device_id_type=MESH)

    @pl.when(is_mid)
    def _():
        pl.semaphore_signal(barrier, inc=1, device_id=far_end, device_id_type=MESH)

    load_s = pltpu.make_async_copy(s_hbm, s_ref, in_sem.at[0])

    def x_copy(h, gg):
        start = (gg * hi + half_of(h) * pair) * lo * block * 2
        return pltpu.make_async_copy(
            x_hbm.at[pl.ds(pl.multiple_of(start, 16), plan.rows_h * 2), :], x_ref.at[h, gg], in_sem.at[2 + h]
        )

    def w_copy(c):
        return pltpu.make_async_copy(w_hbm.at[:, pl.ds(c * cols, cols)], wbuf.at[c, 0], in_sem.at[4 if c else 1])

    w_copy(0).start()
    load_s.start()
    for gg in range(plan.grp):
        x_copy(0, gg).start()
    for c in range(1, chunks):
        w_copy(c).start()
    for gg in range(plan.grp):
        x_copy(1, gg).start()
    load_list = pltpu.make_async_copy(list_hbm, list_ref, list_sem)
    load_list.start()

    contract = (((1,), (1,)), ((), ()))

    def stack():
        load_s.wait()
        upper = s_ref[...]
        both_buf[...] = jnp.concatenate([upper, -upper[half:], upper[:half]], axis=0)

    def partial(h):
        both = both_buf[...]
        arrived(x_ref.at[h], in_sem.at[2 + h])
        for gg in range(plan.grp):
            value = lax.dot_general(x_ref[h, gg], both, contract, preferred_element_type=F32)
            b = gg % 2
            even_buf[b] = value[:, :width]
            odd_buf[b] = value[:, width:]
            value = (
                even_buf[b, pl.ds(0, plan.rows_h, stride=2), :] + odd_buf[b, pl.ds(1, plan.rows_h, stride=2), :]
            )
            pall[h, gg] = value.reshape(pair, lo, block, width).astype(BF16)

    def remote(src, dst, send, recv, target):
        return pltpu.make_async_remote_copy(
            src_ref=src, dst_ref=dst, send_sem=send, recv_sem=recv, device_id=target, device_id_type=MESH
        )

    def arrived(ref, sem):
        pltpu.make_async_copy(ref, ref, sem).wait()

    def send_w(c):
        if c == 0:
            w_copy(0).wait()
        if c == 1:
            arrived(wbuf.at[pl.ds(1, chunks - 1), 0], in_sem.at[4])
        for o in sorted(range(count), key=lambda o: -hops(o)):
            if o == 0 and cores == 1:
                continue
            dc = cores - 1
            gg, yy = peer(*offsets[o], dc)
            k = slot(o, dc)
            sem = wrecv.at[c, 1 if o == 0 else 0]
            remote(wbuf.at[c, 0], wbuf.at[c, k], send_sem.at[0], sem, (gg, z * lo + yy)).start()

    def relay_w(c):
        arrived(wbuf.at[c, pl.ds(slot(1, cores - 1), count - 1)], wrecv.at[c, 0])
        if cores == 1:
            return
        gg, yy = peer(0, 0, 1)
        for o in range(1, count):
            source = wbuf.at[c, slot(o, 1)]
            remote(source, wbuf.at[c, o], send_sem.at[0], wrecv.at[c, 1], (gg, z * lo + yy)).start()

    def ready_w(c):
        if cores > 1:
            arrived(wbuf.at[c, pl.ds(1, count)], wrecv.at[c, 1])

    def send_p(h):
        for o, dc in plane:
            gg, yy = peer(*offsets[o], dc)
            k = slot(o, dc)
            source = pall.at[h, gg, :, yy]
            remote(source, pbuf.at[h, k], send_sem.at[1], precv.at[h], (gg, z * lo + yy)).start()

    sign = jnp.where(lax.broadcasted_iota(jnp.int32, (block, width), 1) < half, 1.0, -1.0).astype(F32)
    orders = ((1 - zh, zh), (1 - zl, zl))

    def place(h, k, rows):
        for i in range(pair):
            row = (h * pair + i) * 2 * block
            part = rows(i).astype(F32)
            columns = pl.ds(k * width, width)
            lhs_buf[pl.ds(row, block), columns] = (part * sign).astype(BF16)
            turned = jnp.concatenate([part[:, half:], part[:, :half]], axis=1)
            lhs_buf[pl.ds(row + block, block), columns] = turned.astype(BF16)

    def wait_p(h):
        place(h, 0, lambda i: pall[h, g, orders[h][i], y])
        arrived(pbuf.at[h, pl.ds(1, plan.slots - 1)], precv.at[h])
        for o, dc in plane:
            k = slot(o, dc)
            place(h, k, lambda i: pbuf[h, k, orders[h][i]])

    def product(h, c):
        weights = wbuf[c].reshape(plan.slots * width, cols)
        left = lhs_buf[pl.ds(h * pair * 2 * block, pair * 2 * block), :]
        return jnp.dot(left, weights, preferred_element_type=F32).reshape(pair, 2, block, cols)

    def to_near(c, i):
        return remote(share_buf.at[c, i], near_buf.at[c, i], send_sem.at[2], nrecv.at[c + i if c == chunks - 1 else c], near)

    def to_owner(c, i):
        target = level((1 - zh) * pair + orders[0][i])
        return remote(share_buf.at[c, i], got_buf.at[c, 1], send_sem.at[2], srecv.at[c], target)

    def to_pair(c):
        return remote(pass_buf.at[c], got_buf.at[c, 0], send_sem.at[3], srecv.at[c], near)

    def first_end(c):
        share_buf[c] = product(0, c).astype(BF16)
        for i in range(pair):
            to_near(c, i).start()

    def first_mid(c):
        own_buf[c] = product(0, c)

    def merge(c):
        if c < chunks - 1:
            arrived(near_buf.at[c], nrecv.at[c])
        for i in range(pair):
            if c == chunks - 1:
                arrived(near_buf.at[c, i], nrecv.at[c + i])
            share_buf[c, i] = (own_buf[c, i] + near_buf[c, i].astype(F32)).astype(BF16)
            to_owner(c, i).start()

    def second(c):
        value = product(1, c)
        pass_buf[c] = value[0].astype(BF16)
        to_pair(c).start()
        last_buf[c] = value[1]

    def finish(c):
        arrived(got_buf.at[c], srecv.at[c])
        total = last_buf[c] + got_buf[c, 1].astype(F32) + got_buf[c, 0].astype(F32)
        rounded = total.astype(BF16).reshape(2 * block, cols)
        placed = jnp.dot(rounded, pick_buf[pl.ds(c * cols, cols), :], preferred_element_type=F32)
        if c == 0:
            acc_buf[...] = placed
        elif c < chunks - 1:
            acc_buf[...] += placed
        else:
            out_ref[...] = (acc_buf[...] + placed).astype(BF16).reshape(2, block, plan.beams)

    pl.semaphore_wait(barrier, len(plane) + jnp.where(is_mid, 3, 2))
    @pl.when(core == 0)
    def _():
        send_w(0)

    stack()
    partial(0)
    send_p(0)

    @pl.when(core != 0)
    def _():
        send_w(0)

    for c in range(1, min(AHEAD, chunks)):
        send_w(c)
    partial(1)
    load_list.wait()
    for c in range(chunks):
        row = lax.broadcasted_iota(jnp.int32, (cols, plan.beams), 0) + c * cols
        pick_buf[pl.ds(c * cols, cols), :] = jnp.where(row == list_ref[...], 1.0, 0.0).astype(BF16)
    actions = {
        "W": send_w,
        "R": relay_w,
        "Y": ready_w,
        "M": merge,
        "P": wait_p,
        "S": second,
    }

    def follow(steps, first):
        for step in steps:
            if step == "X":
                send_p(1)
            elif step[0] == "F":
                first(int(step[1:]))
            else:
                actions[step[0]](int(step[1:]))

    @pl.when(is_end)
    def _():
        follow(plan.steps(END), first_end)

    @pl.when(is_mid)
    def _():
        follow(plan.steps(MID), first_mid)

    arrived(wbuf.at[:, pl.ds(1, plan.slots - 1)], send_sem.at[0])
    arrived(pbuf.at[:, pl.ds(1, plan.slots - 1)], send_sem.at[1])
    for c in range(chunks):
        if c == chunks - 1:
            arrived(share_buf, send_sem.at[2])
            arrived(pass_buf, send_sem.at[3])
        finish(c)


def shards(plan, snapshots, steering, combining, beam_list):
    snap, _, _, elements = snapshots.shape
    signal = snapshots.reshape(snap * 2, elements)
    steer = jnp.transpose(steering[0], (0, 2, 1)).reshape(plan.width, elements)
    weights = combining.reshape(plan.width, plan.beams)
    pair, block, cols, chunks, halves = plan.pair, plan.block, plan.cols, plan.chunks, plan.halves
    hbm = pl.BlockSpec(memory_space=pl.ANY)
    dma = pltpu.SemaphoreType.DMA
    return pl.pallas_call(
        functools.partial(beam_kernel, plan),
        out_shape=pltpu.VMEM((2, block, plan.beams), BF16),
        in_specs=[hbm, hbm, hbm, hbm],
        out_specs=pl.BlockSpec(memory_space=pltpu.VMEM),
        scratch_shapes=[
            pltpu.VMEM((halves, plan.grp, plan.rows_h * 2, elements), BF16),
            pltpu.VMEM((plan.width, elements), BF16),
            pltpu.VMEM((2 * plan.width, elements), BF16),
            pltpu.VMEM((1, plan.beams), jnp.int32),
            dma((5,)),
            dma(()),
            pltpu.VMEM((2, plan.rows_h * 2, plan.width), F32),
            pltpu.VMEM((2, plan.rows_h * 2, plan.width), F32),
            pltpu.VMEM((halves, plan.grp, pair, plan.lo, block, plan.width), BF16),
            pltpu.VMEM((halves, plan.slots, pair, block, plan.width), BF16),
            pltpu.VMEM((halves * pair * 2 * block, plan.slots * plan.width), BF16),
            pltpu.VMEM((chunks, plan.slots, plan.width, cols), BF16),
            pltpu.VMEM((chunks, pair, 2, block, cols), F32),
            pltpu.VMEM((chunks, pair, 2, block, cols), BF16),
            pltpu.VMEM((chunks, 2, block, cols), BF16),
            pltpu.VMEM((chunks, 2, block, cols), F32),
            pltpu.VMEM((chunks, pair, 2, block, cols), BF16),
            pltpu.VMEM((chunks, 2, 2, block, cols), BF16),
            pltpu.VMEM((plan.beams, plan.beams), BF16),
            pltpu.VMEM((2 * block, plan.beams), F32),
            dma((4,)),
            dma((halves,)),
            dma((chunks, 2)),
            dma((chunks,)),
            dma((chunks + 1,)),
        ],
        compiler_params=pltpu.CompilerParams(
            collective_id=0, has_side_effects=True, vmem_limit_bytes=VMEM_LIMIT
        ),
    )(signal, steer, weights, beam_list.reshape(1, plan.beams))


def solution(mesh):
    placed = (
        P(None, None, ("grp", "sub"), None),
        P(("grp", "sub"), None, None, None),
        P(("grp", "sub"), None, None, None),
        P(),
    )

    def whole(snapshots, steering, combining, beam_list):
        plan = Plan(mesh, snapshots.shape[0], 2 * steering.shape[3], combining.shape[3])
        return jax.shard_map(
            functools.partial(shards, plan),
            mesh=mesh,
            in_specs=placed,
            out_specs=P(None, ("grp", "sub"), None),
            check_vma=False,
        )(snapshots, steering, combining, beam_list)

    return whole
```
